32 devices in a mesh: az: 4 (over y, x), rad: 8 (over z, core).
Axes of the slice: x: 2, y: 2, z: 4, core: 2. Of those that a mesh axis runs over, the one named last changes fastest.
Arguments:
- fields: float32 [5, 96, 32, 512], P(None, 'rad', None, 'az'), may hold values from -6 to 6
- shift: int32 [96], replicated, may hold values from 0 to 511
- fraction: float32 [96], replicated, may hold values from -0.5 to 0.5
- radial_rate: float32 [96, 32], replicated, may hold values from -0.4 to 0.4
Outputs:
- updated: float32 [5, 96, 32, 512], P(None, 'rad', None, 'az')
The draws below stay inside these ranges and needn't reach their ends.
All inputs are finite; a program needn't handle non-finite values.
Results may differ from the reference program's by a relative error of at most 0.0003.
Values sent between devices are 32-bit elements; how exact they have to be, the bound alone decides.
No kernel may reach another device: no remote copies, remote signals or barrier semaphores. Data moves between devices by JAX's collectives and lax.ppermute only.
A program may use at most 64 MiB of HBM per device.

```python
import jax
import jax.numpy as jnp
from jax import lax

NP = 32
NF = 5
NA = 512
NR = 96


def touch_ends(entries, rng, low, largest):
    extent = entries.shape
    index_at = [jax.random.randint(jax.random.fold_in(rng, axis), (), 0, extent[axis]) for axis in range(len(extent))]
    entries = entries.at[tuple(index_at)].set(low)
    longest = extent.index(max(extent))
    index_at[longest] = (index_at[longest] + 1) % extent[longest]
    return entries.at[tuple(index_at)].set(largest)


def level_of(key, shape, cuts, low, high):
    level, own = 1.0, jax.random.fold_in(key, 6)
    for dim, shards_of in cuts:
        steps = jnp.exp(jax.random.uniform(jax.random.fold_in(own, dim), (shards_of,), jnp.float32, low / len(cuts), high / len(cuts)))
        level = level * jnp.repeat(steps, shape[dim] // shards_of).reshape([-1 if axis == dim else 1 for axis in range(len(shape))])
    return level


def gaussian(key, dims, scale, reach, pieces=(), kind=jnp.bfloat16):
    entries = scale * jax.random.normal(key, dims, jnp.float32)
    if pieces:
        entries = entries * level_of(key, dims, pieces, -0.22, 0.18)
    return jnp.clip(entries, -reach, reach).astype(kind)


def setup_inputs(seed: int = 0) -> dict:
    splits = jax.random.split(jax.random.key(seed), 5)
    fields = gaussian(splits[0], (NF, NR, NP, NA), 1.0, 6.0, ((1, 8), (3, 4)), jnp.float32)
    shift = touch_ends(jax.random.randint(splits[1], (NR,), 0, NA), jax.random.fold_in(splits[1], 1), 0, NA - 1).astype(jnp.int32)
    fraction = jnp.clip(jax.random.uniform(splits[2], (NR,), jnp.float32, -0.5, 0.5), -0.5, 0.5)
    radial_rate = jnp.clip(jax.random.uniform(splits[3], (NR, NP), jnp.float32, -0.4, 0.4), -0.4, 0.4)
    return {"fields": fields, "shift": shift, "fraction": fraction, "radial_rate": radial_rate}


def cut(values, low, count, axis):
    return lax.slice_in_dim(values, low, low + count, axis=axis)


def limited(left, right):
    steep = jnp.minimum(jnp.minimum(2.0 * jnp.abs(left), 2.0 * jnp.abs(right)), 0.5 * jnp.abs(left + right))
    return jnp.where(left * right > 0.0, jnp.sign(left) * steep, 0.0)


def flux_change(padded, courant, axis):
    count = padded.shape[axis] - 4
    left = cut(padded, 1, count + 2, axis) - cut(padded, 0, count + 2, axis)
    right = cut(padded, 2, count + 2, axis) - cut(padded, 1, count + 2, axis)
    slope = limited(left, right)
    forward = cut(padded, 1, count + 1, axis) + 0.5 * (1.0 - courant) * cut(slope, 0, count + 1, axis)
    backward = cut(padded, 2, count + 1, axis) - 0.5 * (1.0 + courant) * cut(slope, 1, count + 1, axis)
    flux = courant * jnp.where(courant > 0.0, forward, backward)
    return cut(flux, 1, count, axis) - cut(flux, 0, count, axis)


def one_field(single, shift, fraction, face_rates):
    rolled = lax.map(lambda item: jnp.roll(item[0], item[1], axis=-1), (single, shift))
    padded = jnp.concatenate([rolled[:, :, -2:], rolled, rolled[:, :, :2]], axis=2)
    azimuthal = rolled - flux_change(padded, fraction[:, None, None], 2)
    zeros = jnp.zeros((2,) + azimuthal.shape[1:], jnp.float32)
    radial = jnp.concatenate([zeros, azimuthal, zeros], axis=0)
    return azimuthal - flux_change(radial, face_rates[:, :, None], 0)


def reference(fields, shift, fraction, radial_rate):
    edge = jnp.zeros((1, radial_rate.shape[1]), jnp.float32)
    face_rates = jnp.concatenate([edge, radial_rate[:-1], edge], axis=0)
    return lax.map(lambda single: one_field(single, shift, fraction, face_rates), fields)
```

```python
import functools

import jax
import jax.numpy as jnp
from jax import lax
from jax.experimental import pallas as pl
from jax.experimental.pallas import tpu as pltpu
from jax.sharding import PartitionSpec as P


def pick(table, position):
    chosen = jnp.int32(table[0])
    for place, entry in enumerate(table[1:], 1):
        chosen = jnp.where(position == place, jnp.int32(entry), chosen)
    return chosen


def limited(left, right):
    bound = jnp.where(
        left * right > 0.0, 2.0 * jnp.minimum(jnp.abs(left), jnp.abs(right)), 0.0
    )
    return jnp.maximum(jnp.minimum(0.5 * (left + right), bound), -bound)


def plan(rows, group):
    edges = [0, 1, rows - 2, rows - 1]
    inner = [row for row in range(rows) if row not in edges]
    first = edges + inner[: group - len(edges)]
    rest = inner[group - len(edges):]
    each = len(rest) // group
    starts = [rest[device * each] for device in range(group)] if each else []
    return first, starts, each


def azimuthal_kernel(starts, rows, shift, fraction, *refs):
    group = len(refs) // 2
    parts, results = (refs[:group], refs[group:])
    fields, count, _, width = parts[0].shape
    cycle = group * width
    first = lax.axis_index("rad") * rows + pick(starts, lax.axis_index("az"))
    for step in range(count):
        move = shift[first + step]
        courant = fraction[first + step]
        ahead = courant > 0.0
        weight = jnp.where(ahead, 0.5 * (1.0 - courant), -0.5 * (1.0 + courant))
        late = jnp.where(ahead, move, lax.rem(move + (cycle - 1), cycle))
        for field in range(fields):
            cells = jnp.concatenate(
                [parts[(group - place) % group][field, step] for place in range(group)], axis=1
            )
            right = pltpu.roll(cells, cycle - 1, 1) - cells
            face = cells + weight * limited(pltpu.roll(right, 1, 1), right)
            change = face - pltpu.roll(face, 1, 1)
            final = pltpu.roll(cells, move, 1) - courant * pltpu.roll(change, late, 1)
            for place in range(group):
                results[place][field, step] = final[:, place * width:(place + 1) * width]


def azimuthal(parts, starts, rows, shift, fraction):
    vmem = pl.BlockSpec(memory_space=pltpu.VMEM)
    smem = pl.BlockSpec(memory_space=pltpu.SMEM)
    return pl.pallas_call(
        functools.partial(azimuthal_kernel, starts, rows),
        out_shape=[jax.ShapeDtypeStruct(part.shape, part.dtype) for part in parts],
        in_specs=[smem, smem] + [vmem] * len(parts),
        out_specs=[vmem] * len(parts),
        name="azimuthal",
    )(shift, fraction, *parts)


def radial_kernel(places, rows, rates, *refs):
    parts, result, cells = (refs[:-2], refs[-2], refs[-1])
    here = lax.axis_index("az")
    for part, place in zip(parts, places):
        start = pick(place, here)
        for step in range(part.shape[1]):
            cells[start + step] = part[0, step]
    before, middle = (cells[0], cells[1])
    left = middle - before
    slope_before = cell_before = flux_before = None
    for row in range(rows + 2):
        after = cells[row + 2]
        right = after - middle
        slope = limited(left, right)
        if row:
            courant = rates[row - 1]
            forward = cell_before + 0.5 * (1.0 - courant) * slope_before
            backward = middle - 0.5 * (1.0 + courant) * slope
            flux = courant * jnp.where(courant > 0.0, forward, backward)
            if row > 1:
                result[0, row - 2] = cell_before - (flux - flux_before)
            flux_before = flux
        slope_before, cell_before, middle, left = (slope, middle, after, right)


def radial(parts, places, rates, rows):
    fields, _, polar, width = parts[0].shape
    spec = lambda count: pl.BlockSpec((1, count, polar, width), lambda field: (field, 0, 0, 0))
    return pl.pallas_call(
        functools.partial(radial_kernel, places, rows),
        grid=(fields,),
        out_shape=jax.ShapeDtypeStruct((fields, rows, polar, width), jnp.float32),
        in_specs=[pl.BlockSpec(rates.shape, lambda field: (0, 0, 0))]
        + [spec(part.shape[1]) for part in parts],
        out_specs=spec(rows),
        scratch_shapes=[pltpu.VMEM((rows + 5, polar, width), jnp.float32)],
        name="radial",
    )(rates, *parts)


def exchange(parts, group):
    moved = [
        lax.ppermute(part, "az", [(i, (i + k) % group) for i in range(group)])
        for k, part in enumerate(parts[1:], 1)
    ]
    return [parts[0]] + moved


def shards(fields, shift, fraction, radial_rate):
    rows, width = (fields.shape[1], fields.shape[3])
    group, blocks = (lax.axis_size("az"), lax.axis_size("rad"))
    here = lax.axis_index("az")
    first, starts, each = plan(rows, group)
    sets = [(first, 1)] + ([(starts, each)] if each else [])

    def cut_for(place, table, count):
        row = jnp.asarray(table, jnp.int32)[(here + place) % group]
        return lax.dynamic_slice_in_dim(fields, row, count, axis=1)

    cycles = [
        exchange([cut_for(k, table, count) for k in range(group)], group) for table, count in sets
    ]
    parts, places = ([], [])
    for (table, count), cycle in zip(sets, cycles):
        updated = exchange(azimuthal(cycle, table, rows, shift, fraction), group)
        for k in range(group):
            parts.append(updated[k])
            places.append([2 + table[(i - k) % group] for i in range(group)])
    for k in range(group):
        pairs, place = ([], [])
        for i in range(group):
            row = first[(i - k) % group]
            step = -1 if row < 2 else 1 if row >= rows - 2 else 0
            place.append({-1: rows + 2 + row, 1: row - (rows - 2), 0: rows + 4}[step])
            if step:
                pairs += [
                    (i * blocks + b, i * blocks + b + step)
                    for b in range(blocks)
                    if 0 <= b + step < blocks
                ]
        parts.append(lax.ppermute(parts[k], ("az", "rad"), pairs))
        places.append(place)
    edge = jnp.zeros((1, radial_rate.shape[1]), jnp.float32)
    extended = jnp.concatenate([edge, radial_rate[:-1], edge], axis=0)
    face_rates = lax.dynamic_slice_in_dim(extended, lax.axis_index("rad") * rows, rows + 1)
    rates = jnp.broadcast_to(face_rates[:, :, None], face_rates.shape + (width,))
    return radial(parts, places, rates, rows)


def solution(mesh):
    placed = (P(None, "rad", None, "az"), P(), P(), P())
    return jax.shard_map(
        shards, mesh=mesh, in_specs=placed, out_specs=P(None, "rad", None, "az"), check_vma=False
    )
```

```python
import functools

import jax
import jax.numpy as jnp
from jax import lax
from jax.experimental import pallas as pl
from jax.experimental.pallas import tpu as pltpu
from jax.sharding import PartitionSpec as P


def pick(table, position):
    chosen = jnp.int32(table[0])
    for place, entry in enumerate(table[1:], 1):
        chosen = jnp.where(position == place, jnp.int32(entry), chosen)
    return chosen


def limited(left, right):
    bound = jnp.where(
        left * right > 0.0, 2.0 * jnp.minimum(jnp.abs(left), jnp.abs(right)), 0.0
    )
    return jnp.maximum(jnp.minimum(0.5 * (left + right), bound), -bound)


def plan(rows, group):
    edges = [0, 1, rows - 2, rows - 1]
    inner = [row for row in range(rows) if row not in edges]
    first = edges + inner[: group - len(edges)]
    rest = inner[group - len(edges):]
    each = len(rest) // group
    starts = [rest[device * each] for device in range(group)] if each else []
    return first, starts, each


def kept(array):
    return pltpu.with_memory_space_constraint(array, pltpu.VMEM)


def pack_kernel(table, fields, *refs):
    group = len(refs) - 1
    results, sems = (refs[:group], refs[group])
    here = lax.axis_index("az")
    copies = []
    for place, result in enumerate(results):
        rotated = [table[(device + place) % group] for device in range(group)]
        source = fields.at[:, pl.ds(pick(rotated, here), result.shape[1])]
        copies.append(pltpu.make_async_copy(source, result, sems.at[place]))
    for copy in copies:
        copy.start()
    for copy in copies:
        copy.wait()


def pack(fields, table, count, group):
    shape = (fields.shape[0], count) + fields.shape[2:]
    return pl.pallas_call(
        functools.partial(pack_kernel, table),
        out_shape=[pltpu.VMEM(shape, fields.dtype)] * group,
        in_specs=[pl.BlockSpec(memory_space=pl.ANY)],
        out_specs=[pl.BlockSpec(memory_space=pltpu.VMEM)] * group,
        scratch_shapes=[pltpu.SemaphoreType.DMA((group,))],
        name="pack",
    )(fields)


def rates_kernel(rows, turned, result):
    columns = turned[...]
    place = lax.broadcasted_iota(jnp.int32, columns.shape, 1)
    inside = jnp.where(place < columns.shape[1] - 1, columns, 0.0)
    below = lax.axis_index("rad") * rows - 1
    for row in range(result.shape[0]):
        column = jnp.sum(
            jnp.where(place == below + row, inside, 0.0), axis=1, keepdims=True
        )
        result[row] = jnp.broadcast_to(column, result.shape[1:])


def spread_rates(radial_rate, rows, width):
    return pl.pallas_call(
        functools.partial(rates_kernel, rows),
        out_shape=pltpu.VMEM((rows + 1, radial_rate.shape[1], width), jnp.float32),
        in_specs=[pl.BlockSpec(memory_space=pltpu.VMEM)],
        out_specs=pl.BlockSpec(memory_space=pltpu.VMEM),
        name="spread_rates",
    )(radial_rate.T)


def azimuthal_kernel(starts, rows, shift, fraction, *refs):
    group = len(refs) // 2
    parts, results = (refs[:group], refs[group:])
    fields, count, _, width = parts[0].shape
    cycle = group * width
    first = lax.axis_index("rad") * rows + pick(starts, lax.axis_index("az"))
    for step in range(count):
        move = shift[first + step]
        courant = fraction[first + step]
        ahead = courant > 0.0
        weight = jnp.where(ahead, 0.5 * (1.0 - courant), -0.5 * (1.0 + courant))
        for field in range(fields):
            cells = jnp.concatenate(
                [parts[(group - place) % group][field, step] for place in range(group)], axis=1
            )
            right = pltpu.roll(cells, cycle - 1, 1) - cells
            face = cells + weight * limited(pltpu.roll(right, 1, 1), right)
            change = face - pltpu.roll(face, 1, 1)
            change = jnp.where(ahead, change, pltpu.roll(change, cycle - 1, 1))
            final = pltpu.roll(cells - courant * change, move, 1)
            for place in range(group):
                results[place][field, step] = final[:, place * width:(place + 1) * width]


def azimuthal(parts, starts, rows, shift, fraction):
    vmem = pl.BlockSpec(memory_space=pltpu.VMEM)
    smem = pl.BlockSpec(memory_space=pltpu.SMEM)
    return pl.pallas_call(
        functools.partial(azimuthal_kernel, starts, rows),
        out_shape=[pltpu.VMEM(part.shape, part.dtype) for part in parts],
        in_specs=[smem, smem] + [vmem] * len(parts),
        out_specs=[vmem] * len(parts),
        name="azimuthal",
    )(shift, fraction, *map(kept, parts))


def radial_kernel(places, rows, rates, *refs):
    count = len(places)
    parts, result, cells, done, sems = (refs[:count],) + refs[count:]
    here = lax.axis_index("az")
    starts = [pick(place, here) for place in places]
    copies = []
    for field in range(parts[0].shape[0]):
        for part, start in zip(parts, starts):
            for step in range(part.shape[1]):
                cells[field, start + step] = part[field, step]
        flow(cells.at[field], rates, done.at[field], rows)
        copies.append(pltpu.make_async_copy(done.at[field], result.at[field], sems.at[field]))
        copies[-1].start()
    for copy in copies:
        copy.wait()


def flow(cells, rates, result, rows):
    before, middle = (cells[0], cells[1])
    left = middle - before
    slope_before = cell_before = flux_before = None
    for row in range(rows + 2):
        after = cells[row + 2]
        right = after - middle
        slope = limited(left, right)
        if row:
            courant = rates[row - 1]
            forward = cell_before + 0.5 * (1.0 - courant) * slope_before
            backward = middle - 0.5 * (1.0 + courant) * slope
            flux = courant * jnp.where(courant > 0.0, forward, backward)
            if row > 1:
                result[row - 2] = cell_before - (flux - flux_before)
            flux_before = flux
        slope_before, cell_before, middle, left = (slope, middle, after, right)


def radial(parts, places, rates, rows):
    fields, _, polar, width = parts[0].shape
    vmem = pl.BlockSpec(memory_space=pltpu.VMEM)
    shape = (fields, rows, polar, width)
    return pl.pallas_call(
        functools.partial(radial_kernel, places, rows),
        out_shape=jax.ShapeDtypeStruct(shape, jnp.float32),
        in_specs=[vmem] * (1 + len(parts)),
        out_specs=pl.BlockSpec(memory_space=pl.ANY),
        scratch_shapes=[
            pltpu.VMEM((fields, rows + 5, polar, width), jnp.float32),
            pltpu.VMEM(shape, jnp.float32),
            pltpu.SemaphoreType.DMA((fields,)),
        ],
        name="radial",
    )(kept(rates), *map(kept, parts))


def exchange(parts, group):
    moved = [
        lax.ppermute(part, "az", [(i, (i + k) % group) for i in range(group)])
        for k, part in enumerate(parts[1:], 1)
    ]
    return [parts[0]] + moved


def shards(fields, shift, fraction, radial_rate):
    rows, width = (fields.shape[1], fields.shape[3])
    group, blocks = (lax.axis_size("az"), lax.axis_size("rad"))
    first, starts, each = plan(rows, group)
    sets = [(first, 1)] + ([(starts, each)] if each else [])
    cycles = [exchange(pack(fields, table, count, group), group) for table, count in sets]
    rates = spread_rates(radial_rate, rows, width)
    parts, places = ([], [])
    for (table, count), cycle in zip(sets, cycles):
        updated = exchange(azimuthal(cycle, table, rows, shift, fraction), group)
        for k in range(group):
            parts.append(updated[k])
            places.append([2 + table[(i - k) % group] for i in range(group)])
    for k in range(group):
        pairs, place = ([], [])
        for i in range(group):
            row = first[(i - k) % group]
            step = -1 if row < 2 else 1 if row >= rows - 2 else 0
            place.append({-1: rows + 2 + row, 1: row - (rows - 2), 0: rows + 4}[step])
            if step:
                pairs += [
                    (i * blocks + b, i * blocks + b + step)
                    for b in range(blocks)
                    if 0 <= b + step < blocks
                ]
        parts.append(lax.ppermute(parts[k], ("az", "rad"), pairs))
        places.append(place)
    return radial(parts, places, rates, rows)


def solution(mesh):
    placed = (P(None, "rad", None, "az"), P(), P(), P())
    return jax.shard_map(
        shards, mesh=mesh, in_specs=placed, out_specs=P(None, "rad", None, "az"), check_vma=False
    )
```

```python
import functools

import jax
import jax.numpy as jnp
from jax import lax
from jax.experimental import pallas as pl
from jax.experimental.pallas import tpu as pltpu
from jax.sharding import PartitionSpec as P


def pick(table, position):
    chosen = jnp.int32(table[0])
    for place, entry in enumerate(table[1:], 1):
        chosen = jnp.where(position == place, jnp.int32(entry), chosen)
    return chosen


def limited(left, right):
    bound = jnp.where(
        left * right > 0.0, 2.0 * jnp.minimum(jnp.abs(left), jnp.abs(right)), 0.0
    )
    return jnp.maximum(jnp.minimum(0.5 * (left + right), bound), -bound)


def plan(rows, group):
    edges = [0, 1, rows - 2, rows - 1]
    inner = [row for row in range(rows) if row not in edges]
    first = edges + inner[: group - len(edges)]
    rest = inner[group - len(edges):]
    each = len(rest) // group
    starts = [rest[device * each] for device in range(group)] if each else []
    return first, starts, each


def kept(array):
    return pltpu.with_memory_space_constraint(array, pltpu.VMEM)


def pack_kernel(table, rows, fields, turned, *refs):
    group = len(table)
    results, rates, sems = (refs[:group], refs[group:-1], refs[-1])
    here = lax.axis_index("az")
    copies = []
    for place, result in enumerate(results):
        rotated = [table[(device + place) % group] for device in range(group)]
        source = fields.at[:, pl.ds(pick(rotated, here), result.shape[1])]
        copies.append(pltpu.make_async_copy(source, result, sems.at[place]))
    for copy in copies:
        copy.start()
    if rates:
        spread_rates(turned, rates[0], lax.axis_index("rad") * rows - 1)
    for copy in copies:
        copy.wait()


def spread_rates(turned, result, below):
    columns = turned[...]
    place = lax.broadcasted_iota(jnp.int32, columns.shape, 1)
    inside = jnp.where(place < columns.shape[1] - 1, columns, 0.0)
    for row in range(result.shape[0]):
        column = jnp.sum(jnp.where(place == below + row, inside, 0.0), axis=1, keepdims=True)
        result[row] = jnp.broadcast_to(column, result.shape[1:])


def pack(fields, radial_rate, table, count, with_rates):
    group, rows = (len(table), fields.shape[1])
    shape = (fields.shape[0], count) + fields.shape[2:]
    kinds = [pltpu.VMEM(shape, fields.dtype)] * group
    kinds += [pltpu.VMEM((rows + 1,) + fields.shape[2:], jnp.float32)] * with_rates
    vmem = pl.BlockSpec(memory_space=pltpu.VMEM)
    return pl.pallas_call(
        functools.partial(pack_kernel, table, rows),
        out_shape=kinds,
        in_specs=[pl.BlockSpec(memory_space=pl.ANY), vmem if with_rates else pl.BlockSpec(memory_space=pl.ANY)],
        out_specs=[vmem] * len(kinds),
        scratch_shapes=[pltpu.SemaphoreType.DMA((group,))],
        name="pack",
    )(fields, radial_rate.T)


def azimuthal_kernel(starts, rows, shift, fraction, *refs):
    group = len(refs) // 2
    parts, results = (refs[:group], refs[group:])
    fields, count, polar, width = parts[0].shape
    cycle = group * width
    first = lax.axis_index("rad") * rows + pick(starts, lax.axis_index("az"))
    for step in range(count):
        move = shift[first + step]
        courant = fraction[first + step]
        ahead = courant > 0.0
        weight = jnp.where(ahead, 0.5 * (1.0 - courant), -0.5 * (1.0 + courant))
        cells = jnp.concatenate(
            [
                parts[(group - place) % group][:, step].reshape(fields * polar, width)
                for place in range(group)
            ],
            axis=1,
        )
        right = pltpu.roll(cells, cycle - 1, 1) - cells
        face = cells + weight * limited(pltpu.roll(right, 1, 1), right)
        change = face - pltpu.roll(face, 1, 1)
        change = jnp.where(ahead, change, pltpu.roll(change, cycle - 1, 1))
        final = pltpu.roll(cells - courant * change, move, 1)
        for place in range(group):
            results[place][:, step] = final[:, place * width:(place + 1) * width].reshape(
                fields, polar, width
            )


def azimuthal(parts, starts, rows, shift, fraction):
    vmem = pl.BlockSpec(memory_space=pltpu.VMEM)
    smem = pl.BlockSpec(memory_space=pltpu.SMEM)
    return pl.pallas_call(
        functools.partial(azimuthal_kernel, starts, rows),
        out_shape=[pltpu.VMEM(part.shape, part.dtype) for part in parts],
        in_specs=[smem, smem] + [vmem] * len(parts),
        out_specs=[vmem] * len(parts),
        name="azimuthal",
    )(shift, fraction, *map(kept, parts))


def radial_kernel(places, rows, rates, *refs):
    count = len(places)
    parts, result, cells, done, sems = (refs[:count],) + refs[count:]
    here = lax.axis_index("az")
    starts = [pick(place, here) for place in places]
    copies = []
    for field in range(parts[0].shape[0]):
        for part, start in zip(parts, starts):
            for step in range(part.shape[1]):
                cells[field, start + step] = part[field, step]
        flow(cells.at[field], rates, done.at[field], rows)
        copies.append(pltpu.make_async_copy(done.at[field], result.at[field], sems.at[field]))
        copies[-1].start()
    for copy in copies:
        copy.wait()


def flow(cells, rates, result, rows):
    before, middle = (cells[0], cells[1])
    left = middle - before
    slope_before = cell_before = flux_before = None
    for row in range(rows + 2):
        after = cells[row + 2]
        right = after - middle
        slope = limited(left, right)
        if row:
            courant = rates[row - 1]
            forward = cell_before + 0.5 * (1.0 - courant) * slope_before
            backward = middle - 0.5 * (1.0 + courant) * slope
            flux = courant * jnp.where(courant > 0.0, forward, backward)
            if row > 1:
                result[row - 2] = cell_before - (flux - flux_before)
            flux_before = flux
        slope_before, cell_before, middle, left = (slope, middle, after, right)


def radial(parts, places, rates, rows):
    fields, _, polar, width = parts[0].shape
    vmem = pl.BlockSpec(memory_space=pltpu.VMEM)
    shape = (fields, rows, polar, width)
    return pl.pallas_call(
        functools.partial(radial_kernel, places, rows),
        out_shape=jax.ShapeDtypeStruct(shape, jnp.float32),
        in_specs=[vmem] * (1 + len(parts)),
        out_specs=pl.BlockSpec(memory_space=pl.ANY),
        scratch_shapes=[
            pltpu.VMEM((fields, rows + 4, polar, width), jnp.float32),
            pltpu.VMEM(shape, jnp.float32),
            pltpu.SemaphoreType.DMA((fields,)),
        ],
        name="radial",
    )(kept(rates), *map(kept, parts))


def edges_kernel(*refs):
    parts, results = (refs[:-2], refs[-2:])
    group, here = (len(parts), lax.axis_index("az"))
    for edge in range(4):
        source = lax.rem(here - edge + group, group)
        for field in range(parts[0].shape[0]):
            chosen = parts[0][field, 0]
            for k in range(1, group):
                chosen = jnp.where(source == k, parts[k][field, 0], chosen)
            results[edge // 2][field, edge % 2] = chosen


def edges(parts):
    fields, _, polar, width = parts[0].shape
    vmem = pl.BlockSpec(memory_space=pltpu.VMEM)
    return pl.pallas_call(
        edges_kernel,
        out_shape=[pltpu.VMEM((fields, 2, polar, width), jnp.float32)] * 2,
        in_specs=[vmem] * len(parts),
        out_specs=[vmem] * 2,
        name="edges",
    )(*map(kept, parts))


def exchange(parts, group):
    moved = [parts[0]]
    for k in range(1, group):
        moved.append(lax.ppermute(parts[k], "az", [(i, (i + k) % group) for i in range(group)]))
    return moved


def substep(fields, shift, fraction, radial_rate):
    rows = fields.shape[1]
    group, blocks = (lax.axis_size("az"), lax.axis_size("rad"))
    first, starts, each = plan(rows, group)
    sets = [(first, 1)] + ([(starts, each)] if each else [])
    cycles = []
    for turn, (table, count) in enumerate(sets):
        last = turn == len(sets) - 1
        packed = pack(fields, radial_rate, table, count, last)
        cycles.append(exchange(packed[:group], group))
    rates = packed[group]
    parts, places = ([], [])
    for (table, count), cycle in zip(sets, cycles):
        updated = azimuthal(cycle, table, rows, shift, fraction)
        parts += exchange(updated, group)
        for k in range(group):
            places.append([2 + table[(i - k) % group] for i in range(group)])
    low, high = edges(parts[:group])
    up = [(b, b + 1) for b in range(blocks - 1)]
    down = [(b, a) for a, b in up]
    parts.append(lax.ppermute(high, "rad", up))
    parts.append(lax.ppermute(low, "rad", down))
    places += [[0] * group, [rows + 2] * group]
    return radial(parts, places, rates, rows)


def solution(mesh):
    placed = (P(None, "rad", None, "az"), P(), P(), P())
    return jax.shard_map(
        substep, mesh=mesh, in_specs=placed, out_specs=P(None, "rad", None, "az"), check_vma=False
    )
```

```python
import functools

import jax
import jax.numpy as jnp
from jax import lax
from jax.experimental import pallas as pl
from jax.experimental.pallas import tpu as pltpu
from jax.sharding import PartitionSpec as P


def pick(table, position):
    chosen = jnp.int32(table[0])
    for place, entry in enumerate(table[1:], 1):
        chosen = jnp.where(position == place, jnp.int32(entry), chosen)
    return chosen


def limited(left, right):
    bound = jnp.where(
        left * right > 0.0, 2.0 * jnp.minimum(jnp.abs(left), jnp.abs(right)), 0.0
    )
    return jnp.maximum(jnp.minimum(0.5 * (left + right), bound), -bound)


def plan(rows, group):
    edges = [0, 1, rows - 2, rows - 1]
    order = edges + [row for row in range(rows) if row not in edges]
    lists = [order[start:start + group] for start in range(0, rows, group)]
    count = len(lists) - len(lists) // 3
    return [part for part in (lists[:count], lists[count:]) if part]


def kept(array):
    return pltpu.with_memory_space_constraint(array, pltpu.VMEM)


def pack_kernel(lists, fields, *refs):
    results, sems = (refs[:-1], refs[-1])
    group, here = (len(results), lax.axis_index("az"))
    copies = []
    for place, result in enumerate(results):
        for step, table in enumerate(lists):
            row = pick([table[(device + place) % group] for device in range(group)], here)
            copies.append(
                pltpu.make_async_copy(fields.at[:, row], result.at[:, step], sems.at[place, step])
            )
    for copy in copies:
        copy.start()
    for copy in copies:
        copy.wait()


def pack(fields, lists, group):
    shape = (fields.shape[0], len(lists)) + fields.shape[2:]
    return pl.pallas_call(
        functools.partial(pack_kernel, lists),
        out_shape=[pltpu.VMEM(shape, fields.dtype)] * group,
        in_specs=[pl.BlockSpec(memory_space=pl.ANY)],
        out_specs=[pl.BlockSpec(memory_space=pltpu.VMEM)] * group,
        scratch_shapes=[pltpu.SemaphoreType.DMA((group, len(lists)))],
        name="pack",
    )(fields)


def rates_kernel(rows, turned, result):
    columns = turned[...]
    place = lax.broadcasted_iota(jnp.int32, columns.shape, 1)
    inside = jnp.where(place < columns.shape[1] - 1, columns, 0.0)
    below = lax.axis_index("rad") * rows - 1
    for row in range(result.shape[0]):
        column = jnp.sum(jnp.where(place == below + row, inside, 0.0), axis=1, keepdims=True)
        result[row] = jnp.broadcast_to(column, result.shape[1:])


def spread_rates(radial_rate, rows, width):
    return pl.pallas_call(
        functools.partial(rates_kernel, rows),
        out_shape=pltpu.VMEM((rows + 1, radial_rate.shape[1], width), jnp.float32),
        in_specs=[pl.BlockSpec(memory_space=pltpu.VMEM)],
        out_specs=pl.BlockSpec(memory_space=pltpu.VMEM),
        name="spread_rates",
    )(radial_rate.T)


def azimuthal_kernel(lists, rows, shift, fraction, *refs):
    group = len(refs) // 2
    parts, results = (refs[:group], refs[group:])
    fields, count, polar, width = parts[0].shape
    cycle = group * width
    for step in range(count):
        row = lax.axis_index("rad") * rows + pick(lists[step], lax.axis_index("az"))
        move, courant = (shift[row], fraction[row])
        ahead = courant > 0.0
        weight = jnp.where(ahead, 0.5 * (1.0 - courant), -0.5 * (1.0 + courant))
        cells = jnp.concatenate(
            [
                parts[(group - place) % group][:, step].reshape(fields * polar, width)
                for place in range(group)
            ],
            axis=1,
        )
        right = pltpu.roll(cells, cycle - 1, 1) - cells
        face = cells + weight * limited(pltpu.roll(right, 1, 1), right)
        change = face - pltpu.roll(face, 1, 1)
        change = jnp.where(ahead, change, pltpu.roll(change, cycle - 1, 1))
        final = pltpu.roll(cells - courant * change, move, 1)
        for place in range(group):
            results[place][:, step] = final[:, place * width:(place + 1) * width].reshape(
                fields, polar, width
            )


def azimuthal(parts, lists, rows, shift, fraction):
    vmem = pl.BlockSpec(memory_space=pltpu.VMEM)
    smem = pl.BlockSpec(memory_space=pltpu.SMEM)
    return pl.pallas_call(
        functools.partial(azimuthal_kernel, lists, rows),
        out_shape=[pltpu.VMEM(part.shape, part.dtype) for part in parts],
        in_specs=[smem, smem] + [vmem] * len(parts),
        out_specs=[vmem] * len(parts),
        name="azimuthal",
    )(shift, fraction, *map(kept, parts))


def radial_kernel(places, rows, rates, *refs):
    count = len(places)
    parts, result, cells, done, sems = (refs[:count],) + refs[count:]
    here = lax.axis_index("az")
    starts = [[pick(table, here) for table in place] for place in places]
    copies = []
    for field in range(parts[0].shape[0]):
        for part, start in zip(parts, starts):
            for step, row in enumerate(start):
                cells[field, row] = part[field, step]
        flow(cells.at[field], rates, done.at[field], rows)
        copies.append(pltpu.make_async_copy(done.at[field], result.at[field], sems.at[field]))
        copies[-1].start()
    for copy in copies:
        copy.wait()


def flow(cells, rates, result, rows):
    before, middle = (cells[0], cells[1])
    left = middle - before
    slope_before = cell_before = flux_before = None
    for row in range(rows + 2):
        after = cells[row + 2]
        right = after - middle
        slope = limited(left, right)
        if row:
            courant = rates[row - 1]
            forward = cell_before + 0.5 * (1.0 - courant) * slope_before
            backward = middle - 0.5 * (1.0 + courant) * slope
            flux = courant * jnp.where(courant > 0.0, forward, backward)
            if row > 1:
                result[row - 2] = cell_before - (flux - flux_before)
            flux_before = flux
        slope_before, cell_before, middle, left = (slope, middle, after, right)


def radial(parts, places, rates, rows):
    fields, _, polar, width = parts[0].shape
    vmem = pl.BlockSpec(memory_space=pltpu.VMEM)
    shape = (fields, rows, polar, width)
    return pl.pallas_call(
        functools.partial(radial_kernel, places, rows),
        out_shape=jax.ShapeDtypeStruct(shape, jnp.float32),
        in_specs=[vmem] * (1 + len(parts)),
        out_specs=pl.BlockSpec(memory_space=pl.ANY),
        scratch_shapes=[
            pltpu.VMEM((fields, rows + 4, polar, width), jnp.float32),
            pltpu.VMEM(shape, jnp.float32),
            pltpu.SemaphoreType.DMA((fields,)),
        ],
        name="radial",
    )(kept(rates), *map(kept, parts))


def edges_kernel(*refs):
    parts, results = (refs[:-2], refs[-2:])
    group, here = (len(parts), lax.axis_index("az"))
    for edge in range(4):
        source = lax.rem(here - edge + group, group)
        for field in range(parts[0].shape[0]):
            chosen = parts[0][field, 0]
            for k in range(1, group):
                chosen = jnp.where(source == k, parts[k][field, 0], chosen)
            results[edge // 2][field, edge % 2] = chosen


def edges(parts):
    fields, _, polar, width = parts[0].shape
    vmem = pl.BlockSpec(memory_space=pltpu.VMEM)
    return pl.pallas_call(
        edges_kernel,
        out_shape=[pltpu.VMEM((fields, 2, polar, width), jnp.float32)] * 2,
        in_specs=[vmem] * len(parts),
        out_specs=[vmem] * 2,
        name="edges",
    )(*map(kept, parts))


def exchange(parts, group):
    moved = [parts[0]]
    for k in range(1, group):
        moved.append(lax.ppermute(parts[k], "az", [(i, (i + k) % group) for i in range(group)]))
    return moved


def substep(fields, shift, fraction, radial_rate):
    rows = fields.shape[1]
    group, blocks = (lax.axis_size("az"), lax.axis_size("rad"))
    sets = plan(rows, group)
    cycles = []
    for lists in sets:
        packed = pack(fields, lists, group)
        cycles.append(exchange(packed, group))
    parts, places = ([], [])
    for lists, cycle in zip(sets, cycles):
        updated = azimuthal(cycle, lists, rows, shift, fraction)
        parts += exchange(updated, group)
        for k in range(group):
            places.append([[2 + table[(i - k) % group] for i in range(group)] for table in lists])
    low, high = edges(parts[:group])
    up = [(b, b + 1) for b in range(blocks - 1)]
    down = [(b, a) for a, b in up]
    parts.append(lax.ppermute(high, "rad", up))
    parts.append(lax.ppermute(low, "rad", down))
    places += [[[0] * group, [1] * group], [[rows + 2] * group, [rows + 3] * group]]
    rates = spread_rates(radial_rate, rows, fields.shape[3])
    return radial(parts, places, rates, rows)


def solution(mesh):
    placed = (P(None, "rad", None, "az"), P(), P(), P())
    return jax.shard_map(
        substep, mesh=mesh, in_specs=placed, out_specs=P(None, "rad", None, "az"), check_vma=False
    )
```

```python
import functools

import jax
import jax.numpy as jnp
from jax import lax
from jax.experimental import pallas as pl
from jax.experimental.pallas import tpu as pltpu
from jax.sharding import PartitionSpec as P


def pick(table, position):
    chosen = jnp.int32(table[0])
    for place, entry in enumerate(table[1:], 1):
        chosen = jnp.where(position == place, jnp.int32(entry), chosen)
    return chosen


def limited(left, right):
    bound = jnp.where(
        left * right > 0.0, 2.0 * jnp.minimum(jnp.abs(left), jnp.abs(right)), 0.0
    )
    return jnp.maximum(jnp.minimum(0.5 * (left + right), bound), -bound)


def plan(rows, group):
    edges = [0, 1, rows - 2, rows - 1]
    order = edges + [row for row in range(rows) if row not in edges]
    lists = [order[start:start + group] for start in range(0, rows, group)]
    return [part for part in (lists[:1], lists[1:]) if part]


def kept(array):
    return pltpu.with_memory_space_constraint(array, pltpu.VMEM)


def pack_kernel(sets, fields, *refs):
    results, sems = (refs[:-1], refs[-1])
    group, here = (len(results) // len(sets), lax.axis_index("az"))
    copies = []
    for turn, lists in enumerate(sets):
        for place in range(group):
            result = results[turn * group + place]
            for step, table in enumerate(lists):
                row = pick([table[(device + place) % group] for device in range(group)], here)
                sem = sems.at[turn, place, step]
                copies.append(
                    pltpu.make_async_copy(fields.at[:, row], result.at[:, step], sem)
                )
    for copy in copies:
        copy.start()
    for copy in copies:
        copy.wait()


def pack(fields, sets, group):
    kinds = []
    for lists in sets:
        shape = (fields.shape[0], len(lists)) + fields.shape[2:]
        kinds += [pltpu.VMEM(shape, fields.dtype)] * group
    longest = max(len(lists) for lists in sets)
    packed = pl.pallas_call(
        functools.partial(pack_kernel, sets),
        out_shape=kinds,
        in_specs=[pl.BlockSpec(memory_space=pl.ANY)],
        out_specs=[pl.BlockSpec(memory_space=pltpu.VMEM)] * len(kinds),
        scratch_shapes=[pltpu.SemaphoreType.DMA((len(sets), group, longest))],
        name="pack",
    )(fields)
    return [packed[turn * group:(turn + 1) * group] for turn in range(len(sets))]


def rates_kernel(rows, turned, result):
    columns = turned[...]
    place = lax.broadcasted_iota(jnp.int32, columns.shape, 1)
    inside = jnp.where(place < columns.shape[1] - 1, columns, 0.0)
    below = lax.axis_index("rad") * rows - 1
    for row in range(result.shape[0]):
        column = jnp.sum(jnp.where(place == below + row, inside, 0.0), axis=1, keepdims=True)
        result[row] = jnp.broadcast_to(column, result.shape[1:])


def spread_rates(radial_rate, rows, width):
    return pl.pallas_call(
        functools.partial(rates_kernel, rows),
        out_shape=pltpu.VMEM((rows + 1, radial_rate.shape[1], width), jnp.float32),
        in_specs=[pl.BlockSpec(memory_space=pltpu.VMEM)],
        out_specs=pl.BlockSpec(memory_space=pltpu.VMEM),
        name="spread_rates",
    )(radial_rate.T)


def azimuthal_kernel(lists, rows, shift, fraction, *refs):
    group = len(refs) // 2
    parts, results = (refs[:group], refs[group:])
    fields, count, polar, width = parts[0].shape
    cycle = group * width
    for step in range(count):
        row = lax.axis_index("rad") * rows + pick(lists[step], lax.axis_index("az"))
        move, courant = (shift[row], fraction[row])
        ahead = courant > 0.0
        weight = jnp.where(ahead, 0.5 * (1.0 - courant), -0.5 * (1.0 + courant))
        cells = jnp.concatenate(
            [
                parts[(group - place) % group][:, step].reshape(fields * polar, width)
                for place in range(group)
            ],
            axis=1,
        )
        right = pltpu.roll(cells, cycle - 1, 1) - cells
        face = cells + weight * limited(pltpu.roll(right, 1, 1), right)
        change = face - pltpu.roll(face, 1, 1)
        change = jnp.where(ahead, change, pltpu.roll(change, cycle - 1, 1))
        final = pltpu.roll(cells - courant * change, move, 1)
        for place in range(group):
            results[place][:, step] = final[:, place * width:(place + 1) * width].reshape(
                fields, polar, width
            )


def azimuthal(parts, lists, rows, shift, fraction):
    vmem = pl.BlockSpec(memory_space=pltpu.VMEM)
    smem = pl.BlockSpec(memory_space=pltpu.SMEM)
    return pl.pallas_call(
        functools.partial(azimuthal_kernel, lists, rows),
        out_shape=[pltpu.VMEM(part.shape, part.dtype) for part in parts],
        in_specs=[smem, smem] + [vmem] * len(parts),
        out_specs=[vmem] * len(parts),
        name="azimuthal",
    )(shift, fraction, *map(kept, parts))


def radial_kernel(places, rows, rates, *refs):
    count = len(places)
    parts, result, cells, done, sems = (refs[:count],) + refs[count:]
    here = lax.axis_index("az")
    starts = [[pick(table, here) for table in place] for place in places]
    copies = []
    for field in range(parts[0].shape[0]):
        for part, start in zip(parts, starts):
            for step, row in enumerate(start):
                cells[field, row] = part[field, step]
        flow(cells.at[field], rates, done.at[field], rows)
        copies.append(pltpu.make_async_copy(done.at[field], result.at[field], sems.at[field]))
        copies[-1].start()
    for copy in copies:
        copy.wait()


def flow(cells, rates, result, rows):
    before, middle = (cells[0], cells[1])
    left = middle - before
    slope_before = cell_before = flux_before = None
    for row in range(rows + 2):
        after = cells[row + 2]
        right = after - middle
        slope = limited(left, right)
        if row:
            courant = rates[row - 1]
            forward = cell_before + 0.5 * (1.0 - courant) * slope_before
            backward = middle - 0.5 * (1.0 + courant) * slope
            flux = courant * jnp.where(courant > 0.0, forward, backward)
            if row > 1:
                result[row - 2] = cell_before - (flux - flux_before)
            flux_before = flux
        slope_before, cell_before, middle, left = (slope, middle, after, right)


def radial(parts, places, rates, rows):
    fields, _, polar, width = parts[0].shape
    vmem = pl.BlockSpec(memory_space=pltpu.VMEM)
    shape = (fields, rows, polar, width)
    return pl.pallas_call(
        functools.partial(radial_kernel, places, rows),
        out_shape=jax.ShapeDtypeStruct(shape, jnp.float32),
        in_specs=[vmem] * (1 + len(parts)),
        out_specs=pl.BlockSpec(memory_space=pl.ANY),
        scratch_shapes=[
            pltpu.VMEM((fields, rows + 4, polar, width), jnp.float32),
            pltpu.VMEM(shape, jnp.float32),
            pltpu.SemaphoreType.DMA((fields,)),
        ],
        name="radial",
    )(kept(rates), *map(kept, parts))


def edges_kernel(*refs):
    parts, results = (refs[:-2], refs[-2:])
    group, here = (len(parts), lax.axis_index("az"))
    for edge in range(4):
        source = lax.rem(here - edge + group, group)
        for field in range(parts[0].shape[0]):
            chosen = parts[0][field, 0]
            for k in range(1, group):
                chosen = jnp.where(source == k, parts[k][field, 0], chosen)
            results[edge // 2][field, edge % 2] = chosen


def edges(parts):
    fields, _, polar, width = parts[0].shape
    vmem = pl.BlockSpec(memory_space=pltpu.VMEM)
    return pl.pallas_call(
        edges_kernel,
        out_shape=[pltpu.VMEM((fields, 2, polar, width), jnp.float32)] * 2,
        in_specs=[vmem] * len(parts),
        out_specs=[vmem] * 2,
        name="edges",
    )(*map(kept, parts))


def exchange(parts, group):
    moved = [parts[0]]
    for k in range(1, group):
        moved.append(lax.ppermute(parts[k], "az", [(i, (i + k) % group) for i in range(group)]))
    return moved


def substep(fields, shift, fraction, radial_rate):
    rows = fields.shape[1]
    group, blocks = (lax.axis_size("az"), lax.axis_size("rad"))
    sets = plan(rows, group)
    packed = pack(fields, sets, group)
    cycles = [exchange(each, group) for each in packed]
    parts, places = ([], [])
    for lists, cycle in zip(sets, cycles):
        updated = azimuthal(cycle, lists, rows, shift, fraction)
        parts += exchange(updated, group)
        for k in range(group):
            places.append([[2 + table[(i - k) % group] for i in range(group)] for table in lists])
    low, high = edges(parts[:group])
    up = [(b, b + 1) for b in range(blocks - 1)]
    down = [(b, a) for a, b in up]
    parts.append(lax.ppermute(high, "rad", up))
    parts.append(lax.ppermute(low, "rad", down))
    places += [[[0] * group, [1] * group], [[rows + 2] * group, [rows + 3] * group]]
    rates = spread_rates(radial_rate, rows, fields.shape[3])
    return radial(parts, places, rates, rows)


def solution(mesh):
    placed = (P(None, "rad", None, "az"), P(), P(), P())
    return jax.shard_map(
        substep, mesh=mesh, in_specs=placed, out_specs=P(None, "rad", None, "az"), check_vma=False
    )
```
